32 devices in a mesh: grp: 4 (over y, x), slab: 8 (over z, core).
Axes of the slice: x: 2, y: 2, z: 4, core: 2. Of those that a mesh axis runs over, the one named last changes fastest.
Arguments:
- velocity: float32 [16, 3, 4, 16384], P(None, None, 'grp', 'slab'), may hold values from -6 to 6
- old_basis: bfloat16 [64, 3, 4, 16384], P(None, None, None, 'slab'), may hold values from -6 to 6
- singular_values: float32 [64], replicated, may hold values from 0.7 to 1.4
- thickness: int32 [4, 8], P('grp', 'slab'), may hold values from 1 to 4, as said below
Outputs:
- gram_matrix: float32 [80, 80], replicated
- new_basis: bfloat16 [64, 3, 4, 16384], P(None, None, None, 'slab')
- offsets: int32 [4, 8], P('grp', 'slab')
The draws below stay inside these ranges and needn't reach their ends.
Inputs may be any that keep to these rules, and one draw needn't show every extreme that they name: `thickness`: the entry at row-major position p differs from 1 + (p * 3) // 32 by at most one. The first entry is 1 and the last is 4.
All inputs are finite; a program needn't handle non-finite values.
Results may differ from the reference program's by a relative error of at most 0.0004.
The reference program's roundings to bfloat16 on the way (of `snapshot_rows`, `basis_rows`, `stacked` and `mixing_rows`) count: a program that leaves them out, or rounds other values in their place, can miss the bound.
Values may be sent and summed in bfloat16 or wider, within the bound.
A program may use at most 64 MiB of HBM per device.

```python
import math
import jax
import jax.numpy as jnp
from jax import lax

RANK = 64
SNAPS = 16
MAXP = 4
PLANE = 512
CELLS = 16384
N_GRP = 4
N_SLAB = 8


def draw_thickness(key, part):
    total_slabs = N_GRP * N_SLAB
    flat_ids = jnp.arange(total_slabs, dtype=jnp.int32)
    ramp = 1 + flat_ids * (MAXP - 1) // total_slabs
    jitter = jax.random.randint(key, (total_slabs,), -1, 2)
    values = jnp.clip(ramp + jitter, 1, MAXP)
    values = jnp.where(flat_ids == 0, 1, values)
    values = jnp.where(flat_ids == total_slabs - 1, MAXP, values)
    return values.reshape(N_GRP, N_SLAB).astype(jnp.int32)


def steps_of(rng, dims, split, smallest, high):
    def one(dim, parts):
        heights = jax.random.uniform(jax.random.fold_in(jax.random.fold_in(rng, 6), dim), (parts,), jnp.float32, smallest / len(split), high / len(split))
        return jnp.repeat(jnp.exp(heights), dims[dim] // parts).reshape((-1,) + (1,) * (len(dims) - dim - 1))

    factor_of = one(*split[0])
    for cut in split[1:]:
        factor_of = factor_of * one(*cut)
    return factor_of


def normal_values(own_key, extent, scale, bound, cuts=(), held_as=jnp.bfloat16):
    entries = jax.random.normal(own_key, extent, jnp.float32) * scale
    if len(cuts) > 0:
        entries = steps_of(own_key, extent, cuts, -0.22, 0.18) * entries
    return jnp.clip(entries, min=-bound, max=bound).astype(held_as)


def setup_inputs(seed: int = 0) -> dict:
    key_list = jax.random.split(jax.random.key(seed), 5)
    velocity = normal_values(key_list[0], (SNAPS, 3, N_GRP, CELLS), 1.0, 6.0, ((2, 4), (3, 8)), jnp.float32)
    old_basis = normal_values(key_list[1], (RANK, 3, N_GRP, CELLS), 1.0, 6.0, ((3, 8),))
    singular_values = jnp.clip(jnp.exp(jax.random.uniform(key_list[2], (RANK,), jnp.float32, math.log(0.7), math.log(1.4))), 0.7, 1.4)
    thickness = draw_thickness(jax.random.fold_in(key_list[4], 71), 0)
    return dict(velocity=velocity, old_basis=old_basis, singular_values=singular_values, thickness=thickness)


def orthonormalize(matrix, rank_count):
    iterate = matrix * (0.5 * rank_count ** 0.5 / jnp.sqrt(jnp.sum(matrix * matrix)))
    for sweep_index in range(4):
        product = jnp.dot(iterate.T, iterate, precision=lax.Precision.HIGHEST)
        iterate = 1.5 * iterate - 0.5 * jnp.dot(iterate, product, precision=lax.Precision.HIGHEST)
    return iterate

def reference(velocity, old_basis, singular_values, thickness):
    capacity = MAXP * PLANE
    cell_ids = jnp.arange(N_SLAB * capacity, dtype=jnp.int32)
    owners = cell_ids // capacity
    plane_ids = cell_ids % capacity // PLANE
    live_masks = plane_ids[None, :] < thickness[:, owners]
    snapshot_rows = jnp.where(live_masks[None, None], velocity.astype(jnp.bfloat16), jnp.zeros((), jnp.bfloat16))
    basis_rows = jnp.where(live_masks[None, None], old_basis, jnp.zeros((), jnp.bfloat16))
    stacked = jnp.concatenate([basis_rows.reshape(RANK, -1), snapshot_rows.reshape(SNAPS, -1)], 0)
    live_total = jnp.sum(thickness).astype(jnp.float32) * PLANE
    scales = jnp.concatenate([singular_values.astype(jnp.float32), jnp.ones((SNAPS,), jnp.float32)])
    raw_gram = lax.dot_general(stacked, stacked, (((1,), (1,)), ((), ())), preferred_element_type=jnp.float32)
    gram_matrix = raw_gram * scales[:, None] * scales[None, :] / (3.0 * live_total)
    mixing = orthonormalize(gram_matrix[:, :RANK], RANK)
    mixing_rows = (mixing * scales[:, None]).T.astype(jnp.bfloat16)
    updated = jnp.dot(mixing_rows, stacked, preferred_element_type=jnp.float32).astype(jnp.bfloat16)
    new_basis = updated.reshape(RANK, 3, N_GRP, N_SLAB * capacity)
    flat_counts = thickness.reshape(-1)
    offsets = (jnp.cumsum(flat_counts) - flat_counts).astype(jnp.int32).reshape(N_GRP, N_SLAB)
    return (gram_matrix, new_basis, offsets)
```

```python
import jax
import jax.numpy as jnp
from jax import lax
from jax.sharding import PartitionSpec as P

PLANE = 512
AXES = ("grp", "slab")


def orthonormalize(matrix, rank_count):
    iterate = matrix * (0.5 * rank_count**0.5 / jnp.sqrt(jnp.sum(matrix * matrix)))
    for sweep_index in range(4):
        product = jnp.dot(iterate.T, iterate, precision=lax.Precision.HIGHEST)
        iterate = 1.5 * iterate - 0.5 * jnp.dot(iterate, product, precision=lax.Precision.HIGHEST)
    return iterate


def per_device(velocity, old_basis, singular_values, thickness):
    capacity = velocity.shape[-1]
    snap_count = velocity.shape[0]
    rank_count = old_basis.shape[0]
    n_grp, n_slab = lax.axis_size("grp"), lax.axis_size("slab")
    grp, slab = lax.axis_index("grp"), lax.axis_index("slab")
    plane_ids = lax.broadcasted_iota(jnp.int32, (1, capacity), 1) // PLANE
    own_mask = plane_ids < thickness
    masked = jnp.where(
        own_mask[None, None], velocity.astype(jnp.bfloat16), jnp.zeros((), jnp.bfloat16)
    )
    all_snaps = lax.all_gather(masked, "grp", axis=2, tiled=True)
    own_basis = lax.dynamic_slice_in_dim(old_basis, grp, 1, 2)
    columns = jnp.where(own_mask[None, None], own_basis, jnp.zeros((), jnp.bfloat16))
    stacked = jnp.concatenate([columns.reshape(rank_count, -1), masked.reshape(snap_count, -1)], 0)
    raw_gram = lax.dot_general(
        stacked, stacked, (((1,), (1,)), ((), ())), preferred_element_type=jnp.float32
    )
    flat = lax.broadcasted_iota(jnp.int32, (n_grp * n_slab,), 0)
    mine = grp * n_slab + slab
    onehot = jnp.where(flat == mine, thickness[0, 0], 0).astype(jnp.float32)
    raw_gram, counts = lax.psum((raw_gram, onehot), AXES)
    live_cells = jnp.sum(counts) * PLANE
    offsets = jnp.sum(jnp.where(flat < mine, counts, 0.0)).astype(jnp.int32).reshape(1, 1)
    scales = jnp.concatenate([singular_values, jnp.ones((snap_count,), jnp.float32)])
    gram_matrix = raw_gram * scales[:, None] * scales[None, :] / (3.0 * live_cells)
    mixing = orthonormalize(gram_matrix[:, :rank_count], rank_count)
    mixing_rows = (mixing * scales[:, None]).T.astype(jnp.bfloat16)
    slab_counts = lax.dynamic_slice_in_dim(counts.reshape(n_grp, n_slab), slab, 1, 1)
    live = plane_ids.astype(jnp.float32) < slab_counts
    everything = jnp.concatenate([old_basis, all_snaps], 0)
    updated = jnp.einsum(
        "ri,icgn->rcgn", mixing_rows, everything, preferred_element_type=jnp.float32
    )
    new_basis = jnp.where(live[None, None], updated, 0.0).astype(jnp.bfloat16)
    return (gram_matrix, new_basis, offsets)


def solution(mesh):
    in_specs = (P(None, None, "grp", "slab"), P(None, None, None, "slab"), P(), P("grp", "slab"))
    out_specs = (P(), P(None, None, None, "slab"), P("grp", "slab"))
    return jax.shard_map(
        per_device, mesh=mesh, in_specs=in_specs, out_specs=out_specs, check_vma=False
    )
```

```python
import functools
import jax
import jax.numpy as jnp
from jax import lax
from jax.experimental import pallas as pl
from jax.experimental.pallas import tpu as pltpu
from jax.sharding import PartitionSpec as P

PLANE = 512
AXES = ("grp", "slab")
MESH = pl.DeviceIdType.MESH
LANES = 128
COUNT_LANE = 32
HIGHEST = lax.Precision.HIGHEST


def stages_of(n_slab, n_grp):
    found = []
    for axis, size, first in (("slab", n_slab, 2), ("grp", n_grp, 4)):
        base, radix = 1, first
        while base < size:
            radix = min(radix, size // base)
            found.append((axis, base, radix))
            base, radix = base * radix, 4
    return found


def partner(axis, base, radix, shift):
    me = {name: lax.axis_index(name) for name in AXES}
    digit = lax.rem(me[axis] // base, radix)
    other = lax.rem(digit + shift, radix)
    me[axis] = me[axis] + (other - digit) * base
    return tuple(me[name] for name in AXES)


def dot(a, b, dims, precision=None):
    return lax.dot_general(
        a, b, (dims, ((), ())), preferred_element_type=jnp.float32, precision=precision
    )


def iota(shape, dim):
    return lax.broadcasted_iota(jnp.int32, shape, dim)


def gram_kernel(
    n_grp, n_slab, stages,
    thick_ref, sv_ref, snaps_ref, basis_ref,
    gram_ref, mixb_ref, mixs_ref, live_ref, offset_ref, all_ref,
    xb, big, small, *rest,
):
    n_st = len(stages)
    slots = rest[:n_st]
    local_sem, v_send, v_recv, st_send, st_recv = rest[n_st:]
    rank, comps = xb.shape[1], xb.shape[0]
    snap = snaps_ref.shape[1]
    planes = xb.shape[3] // PLANE
    wide = rank * n_grp
    grp, slab = lax.axis_index("grp"), lax.axis_index("slab")

    loads = []
    for c in range(comps):
        load = pltpu.make_async_copy(basis_ref.at[:, c], xb.at[c], local_sem.at[c])
        load.start()
        loads.append(load)
    barrier = pltpu.get_barrier_semaphore()
    greeted = 0
    for axis, base, radix in stages:
        for shift in range(1, radix):
            pl.semaphore_signal(
                barrier, inc=1, device_id=partner(axis, base, radix, shift), device_id_type=MESH
            )
            greeted += 1
    keep = pltpu.make_async_copy(snaps_ref, all_ref.at[grp], local_sem.at[comps])
    keep.start()
    pl.semaphore_wait(barrier, greeted)
    sends = []
    for shift in range(1, n_grp):
        send = pltpu.make_async_remote_copy(
            src_ref=snaps_ref, dst_ref=all_ref.at[grp],
            send_sem=v_send.at[shift - 1], recv_sem=v_recv.at[shift - 1],
            device_id=partner("grp", 1, n_grp, shift), device_id_type=MESH,
        )
        send.start()
        sends.append(send)

    thick = thick_ref[0, 0]
    big[...] = jnp.zeros_like(big)
    small[...] = jnp.zeros_like(small)
    for c in range(comps):
        loads[c].wait()
        for p in range(planes):
            live = jnp.where(p < thick, 1.0, 0.0)
            x = xb[c, :, :, pl.ds(p * PLANE, PLANE)].reshape(wide, PLANE)
            s = snaps_ref[c, :, pl.ds(p * PLANE, PLANE)]
            big[:wide] += live * dot(x, x, ((1,), (1,)))
            big[wide:] += live * dot(s, x, ((1,), (1,)))
            small[...] += live * dot(s, s, ((1,), (1,)))
    pick = jnp.where(iota((rank, wide), 1) == iota((rank, wide), 0) * n_grp + grp, 1.0, 0.0)
    right = dot(big[...], pick, ((1,), (1,)), HIGHEST)
    bb = dot(pick, right[:wide], ((1,), (0,)), HIGHEST)
    sb = right[wide:]
    ss = small[...]
    half, quarter = rank // 2, snap // 2
    rows = half + 2 * quarter
    place = iota((quarter, LANES), 1) - COUNT_LANE
    place = jnp.where(place >= 0, place * quarter + iota((quarter, LANES), 0), -1)
    me = grp * n_slab + slab
    tail = jnp.where(place == me, thick.astype(jnp.float32), 0.0)
    spare = jnp.zeros((quarter, LANES - 2 * snap), jnp.float32)
    tail = tail + jnp.concatenate([ss[:quarter], ss[quarter:], spare], 1)
    total = jnp.concatenate(
        [
            jnp.concatenate([bb[:half], bb[half:]], 1),
            jnp.concatenate([sb[:quarter], sb[quarter:]], 1),
            tail,
        ],
        0,
    )
    sv_row = sv_ref[...]
    eye = iota((rank, rank), 0) == iota((rank, rank), 1)
    sv_col = jnp.sum(jnp.where(eye, sv_row, 0.0), axis=1, keepdims=True)

    at = 0
    for (axis, base, radix), slot in zip(stages, slots):
        digit = lax.rem(lax.axis_index(axis) // base, radix)
        slot[digit] = total
        moves = []
        for shift in range(1, radix):
            move = pltpu.make_async_remote_copy(
                src_ref=slot.at[digit], dst_ref=slot.at[digit],
                send_sem=st_send.at[at], recv_sem=st_recv.at[at],
                device_id=partner(axis, base, radix, shift), device_id_type=MESH,
            )
            move.start()
            moves.append(move)
            at += 1
        for move in moves:
            move.wait()
        total = slot[0]
        for k in range(1, radix):
            total = total + slot[k]

    tail = total[half + quarter :]
    counts = jnp.where(place >= 0, tail, 0.0)
    live_cells = jnp.sum(counts, keepdims=True) * PLANE
    factor = 1.0 / (3.0 * live_cells)
    offset_ref[...] = jnp.sum(jnp.where(place < me, counts, 0.0), keepdims=True).astype(jnp.int32)
    live = jnp.zeros((wide, LANES), jnp.float32)
    region = lax.rem(iota((wide, LANES), 0), n_grp)
    for g in range(n_grp):
        here = jnp.sum(jnp.where(place == g * n_slab + slab, counts, 0.0), keepdims=True)
        live = jnp.where(region == g, here, live)
    live_ref[...] = live

    bb = jnp.concatenate([total[:half, :rank], total[:half, rank:]], 0)
    sb = total[half : half + quarter]
    sb = jnp.concatenate([sb[:, :rank], sb[:, rank:]], 0)
    ss = jnp.concatenate([tail[:, :snap], tail[:, snap : 2 * snap]], 0)
    bb = bb * sv_col * sv_row * factor
    sb = sb * sv_row * factor
    ss = ss * factor
    gram_ref[:rank, :rank] = bb
    gram_ref[rank:, :rank] = sb
    gram_ref[:rank, rank:] = sb.T
    gram_ref[rank:, rank:] = ss
    y = jnp.concatenate([bb, sb], 0)
    y = y * (0.5 * rank**0.5 * lax.rsqrt(jnp.sum(y * y, keepdims=True)))
    for sweep in range(4):
        product = dot(y, y, ((0,), (0,)), HIGHEST)
        y = 1.5 * y - 0.5 * dot(y, product, ((1,), (0,)), HIGHEST)
    yb = (y[:rank] * sv_col).astype(jnp.bfloat16)
    ys = y[rank:].astype(jnp.bfloat16)
    spread = jnp.where(iota((rank, wide), 1) // n_grp == iota((rank, wide), 0), 1.0, 0.0)
    spread = spread.astype(jnp.bfloat16)
    left_b = dot(spread, yb, ((0,), (1,))).astype(jnp.bfloat16)
    both = dot(left_b, spread, ((1,), (0,)))
    same = lax.rem(iota((wide, wide), 0), n_grp) == lax.rem(iota((wide, wide), 1), n_grp)
    mixb_ref[...] = jnp.where(same, both, 0.0).astype(jnp.bfloat16)
    reps = n_grp * snap
    fill = jnp.where(lax.rem(iota((snap, reps), 1), snap) == iota((snap, reps), 0), 1.0, 0.0)
    left_s = dot(spread, ys, ((0,), (1,))).astype(jnp.bfloat16)
    many = dot(left_s, fill.astype(jnp.bfloat16), ((1,), (0,)))
    same = lax.rem(iota((wide, reps), 0), n_grp) == iota((wide, reps), 1) // snap
    mixs_ref[...] = jnp.where(same, many, 0.0).astype(jnp.bfloat16)

    keep.wait()
    for send in sends:
        send.wait()


def update_kernel(live_ref, mixb_ref, mixs_ref, basis_ref, snaps_ref, out_ref):
    rank, _, n_grp, cells = basis_ref.shape
    x = basis_ref[...].reshape(rank * n_grp, cells)
    s = snaps_ref[...].reshape(-1, cells)
    new = dot(mixb_ref[...], x, ((1,), (0,))) + dot(mixs_ref[...], s, ((1,), (0,)))
    p = pl.program_id(1).astype(jnp.float32)
    new = jnp.where(p < live_ref[:, :1], new, 0.0).astype(jnp.bfloat16)
    out_ref[...] = new.reshape(out_ref.shape)


def per_device(velocity, old_basis, singular_values, thickness):
    snap, comps, _, capacity = velocity.shape
    rank, n_grp = old_basis.shape[0], old_basis.shape[2]
    n_slab = lax.axis_size("slab")
    planes = capacity // PLANE
    wide, reps = rank * n_grp, n_grp * snap
    stages = stages_of(n_slab, n_grp)
    moves = sum(radix - 1 for _, _, radix in stages)
    rows = rank // 2 + snap
    snaps = velocity[:, :, 0].astype(jnp.bfloat16).transpose(1, 0, 2)
    vmem = pl.BlockSpec(memory_space=pltpu.VMEM)
    hbm = pl.BlockSpec(memory_space=pl.ANY)
    gram_matrix, mix_b, mix_s, live, offsets, all_snaps = pl.pallas_call(
        functools.partial(gram_kernel, n_grp, n_slab, stages),
        out_shape=(
            jax.ShapeDtypeStruct((rank + snap, rank + snap), jnp.float32),
            jax.ShapeDtypeStruct((wide, wide), jnp.bfloat16),
            jax.ShapeDtypeStruct((wide, reps), jnp.bfloat16),
            jax.ShapeDtypeStruct((wide, LANES), jnp.float32),
            jax.ShapeDtypeStruct((1, 1), jnp.int32),
            jax.ShapeDtypeStruct((n_grp, comps, snap, capacity), jnp.bfloat16),
        ),
        in_specs=[pl.BlockSpec(memory_space=pltpu.SMEM), vmem, vmem, hbm],
        out_specs=(vmem, vmem, vmem, vmem, vmem, hbm),
        scratch_shapes=[
            pltpu.VMEM((comps, rank, n_grp, capacity), jnp.bfloat16),
            pltpu.VMEM((wide + snap, wide), jnp.float32),
            pltpu.VMEM((snap, snap), jnp.float32),
            *[pltpu.VMEM((radix, rows, LANES), jnp.float32) for _, _, radix in stages],
            pltpu.SemaphoreType.DMA((comps + 1,)),
            pltpu.SemaphoreType.DMA((n_grp - 1,)),
            pltpu.SemaphoreType.DMA((n_grp - 1,)),
            pltpu.SemaphoreType.DMA((moves,)),
            pltpu.SemaphoreType.DMA((moves,)),
        ],
        compiler_params=pltpu.CompilerParams(collective_id=0, has_side_effects=True),
        name="gram_exchange",
    )(thickness, singular_values.reshape(1, rank), snaps, old_basis)
    new_basis = pl.pallas_call(
        update_kernel,
        out_shape=jax.ShapeDtypeStruct(old_basis.shape, jnp.bfloat16),
        grid=(comps, planes),
        in_specs=[
            pl.BlockSpec((wide, LANES), lambda c, p: (0, 0)),
            pl.BlockSpec((wide, wide), lambda c, p: (0, 0)),
            pl.BlockSpec((wide, reps), lambda c, p: (0, 0)),
            pl.BlockSpec((rank, 1, n_grp, PLANE), lambda c, p: (0, c, 0, p)),
            pl.BlockSpec((n_grp, 1, snap, PLANE), lambda c, p: (0, c, 0, p)),
        ],
        out_specs=pl.BlockSpec((rank, 1, n_grp, PLANE), lambda c, p: (0, c, 0, p)),
        name="basis_update",
    )(live, mix_b, mix_s, old_basis, all_snaps)
    return (gram_matrix, new_basis, offsets)


def solution(mesh):
    in_specs = (P(None, None, "grp", "slab"), P(None, None, None, "slab"), P(), P("grp", "slab"))
    out_specs = (P(), P(None, None, None, "slab"), P("grp", "slab"))
    return jax.shard_map(
        per_device, mesh=mesh, in_specs=in_specs, out_specs=out_specs, check_vma=False
    )
```

```python
import functools
import jax
import jax.numpy as jnp
from jax import lax
from jax.experimental import pallas as pl
from jax.experimental.pallas import tpu as pltpu
from jax.sharding import PartitionSpec as P

PLANE = 512
AXES = ("grp", "slab")
MESH = pl.DeviceIdType.MESH
LANES = 128
COUNT_LANE = 32
HIGHEST = lax.Precision.HIGHEST


def stages_of(n_slab, n_grp):
    found = []
    for axis, size, first in (("slab", n_slab, 2), ("grp", n_grp, 4)):
        base, radix = 1, first
        while base < size:
            radix = min(radix, size // base)
            found.append((axis, base, radix))
            base, radix = base * radix, 4
    return found


def partner(axis, base, radix, shift):
    me = {name: lax.axis_index(name) for name in AXES}
    digit = lax.rem(me[axis] // base, radix)
    other = lax.rem(digit + shift, radix)
    me[axis] = me[axis] + (other - digit) * base
    return tuple(me[name] for name in AXES)


def dot(a, b, dims, precision=None):
    return lax.dot_general(
        a, b, (dims, ((), ())), preferred_element_type=jnp.float32, precision=precision
    )


def iota(shape, dim):
    return lax.broadcasted_iota(jnp.int32, shape, dim)


def gram_kernel(
    n_grp, n_slab, stages,
    thick_ref, sv_ref, vel_ref, basis_ref,
    gram_ref, mixb_ref, mixs_ref, live_ref, offset_ref, all_ref,
    xb, snaps_ref, big, small, *rest,
):
    n_st = len(stages)
    slots = rest[:n_st]
    local_sem, v_send, v_recv, st_send, st_recv = rest[n_st:]
    rank, comps = xb.shape[1], xb.shape[0]
    snap = snaps_ref.shape[1]
    planes = xb.shape[3] // PLANE
    wide = rank * n_grp
    grp, slab = lax.axis_index("grp"), lax.axis_index("slab")

    loads = []
    for c in range(comps):
        load = pltpu.make_async_copy(basis_ref.at[:, c], xb.at[c], local_sem.at[c])
        load.start()
        loads.append(load)
    barrier = pltpu.get_barrier_semaphore()
    greeted = 0
    for axis, base, radix in stages:
        for shift in range(1, radix):
            pl.semaphore_signal(
                barrier, inc=1, device_id=partner(axis, base, radix, shift), device_id_type=MESH
            )
            greeted += 1
    for c in range(comps):
        snaps_ref[c] = vel_ref[:, c, 0, :].astype(jnp.bfloat16)
    keep = pltpu.make_async_copy(snaps_ref, all_ref.at[grp], local_sem.at[comps])
    keep.start()
    pl.semaphore_wait(barrier, greeted)
    sends = []

    def send_snaps(c):
        for shift in range(1, n_grp):
            at = c * (n_grp - 1) + shift - 1
            send = pltpu.make_async_remote_copy(
                src_ref=snaps_ref.at[c], dst_ref=all_ref.at[grp, c],
                send_sem=v_send.at[at], recv_sem=v_recv.at[at],
                device_id=partner("grp", 1, n_grp, shift), device_id_type=MESH,
            )
            send.start()
            sends.append(send)

    for c in range(comps - 1):
        send_snaps(c)

    thick = thick_ref[0, 0]
    big[...] = jnp.zeros_like(big)
    small[...] = jnp.zeros_like(small)
    for c in range(comps):
        loads[c].wait()
        for p in range(planes):
            live = jnp.where(p < thick, 1.0, 0.0)
            x = xb[c, :, :, pl.ds(p * PLANE, PLANE)].reshape(wide, PLANE)
            s = snaps_ref[c, :, pl.ds(p * PLANE, PLANE)]
            by_basis = live * dot(x, x, ((1,), (1,)))
            by_snaps = live * dot(s, x, ((1,), (1,)))
            for h in range(wide // LANES):
                big[h, :wide] += by_basis[:, h * LANES : (h + 1) * LANES]
                big[h, wide:] += by_snaps[:, h * LANES : (h + 1) * LANES]
            small[...] += live * dot(s, s, ((1,), (1,)))
    pick = jnp.where(iota((rank, wide), 1) == iota((rank, wide), 0) * n_grp + grp, 1.0, 0.0)
    mine = [
        jnp.concatenate([big[h, pl.ds(grp, rank, stride=n_grp), :], big[h, wide:]], 0)
        for h in range(wide // LANES)
    ]
    mine = jnp.concatenate(mine, 1)
    right = dot(mine, pick, ((1,), (1,)), HIGHEST)
    bb, sb = right[:rank], right[rank:]
    ss = small[...]
    half, quarter = rank // 2, snap // 2
    rows = half + 2 * quarter
    place = iota((quarter, LANES), 1) - COUNT_LANE
    place = jnp.where(place >= 0, place * quarter + iota((quarter, LANES), 0), -1)
    me = grp * n_slab + slab
    tail = jnp.where(place == me, thick.astype(jnp.float32), 0.0)
    spare = jnp.zeros((quarter, LANES - 2 * snap), jnp.float32)
    tail = tail + jnp.concatenate([ss[:quarter], ss[quarter:], spare], 1)
    total = jnp.concatenate(
        [
            jnp.concatenate([bb[:half], bb[half:]], 1),
            jnp.concatenate([sb[:quarter], sb[quarter:]], 1),
            tail,
        ],
        0,
    )
    sv_row = sv_ref[...]
    eye = iota((rank, rank), 0) == iota((rank, rank), 1)
    sv_col = jnp.sum(jnp.where(eye, sv_row, 0.0), axis=1, keepdims=True)

    at = 0
    for (axis, base, radix), slot in zip(stages, slots):
        digit = lax.rem(lax.axis_index(axis) // base, radix)
        slot[digit] = total
        moves = []
        for shift in range(1, radix):
            move = pltpu.make_async_remote_copy(
                src_ref=slot.at[digit], dst_ref=slot.at[digit],
                send_sem=st_send.at[at], recv_sem=st_recv.at[at],
                device_id=partner(axis, base, radix, shift), device_id_type=MESH,
            )
            move.start()
            moves.append(move)
            at += 1
        if axis == "grp":
            send_snaps(comps - 1)
        for move in moves:
            move.wait()
        total = slot[0]
        for k in range(1, radix):
            total = total + slot[k]

    tail = total[half + quarter :]
    counts = jnp.where(place >= 0, tail, 0.0)
    live_cells = jnp.sum(counts, keepdims=True) * PLANE
    factor = 1.0 / (3.0 * live_cells)
    offset_ref[...] = jnp.sum(jnp.where(place < me, counts, 0.0), keepdims=True).astype(jnp.int32)
    live = jnp.zeros((wide, LANES), jnp.float32)
    region = lax.rem(iota((wide, LANES), 0), n_grp)
    for g in range(n_grp):
        here = jnp.sum(jnp.where(place == g * n_slab + slab, counts, 0.0), keepdims=True)
        live = jnp.where(region == g, here, live)
    live_ref[...] = live

    bb = jnp.concatenate([total[:half, :rank], total[:half, rank:]], 0)
    sb = total[half : half + quarter]
    sb = jnp.concatenate([sb[:, :rank], sb[:, rank:]], 0)
    ss = jnp.concatenate([tail[:, :snap], tail[:, snap : 2 * snap]], 0)
    bb = bb * sv_col * sv_row * factor
    sb = sb * sv_row * factor
    ss = ss * factor
    gram_ref[:rank, :rank] = bb
    gram_ref[rank:, :rank] = sb
    gram_ref[:rank, rank:] = sb.T
    gram_ref[rank:, rank:] = ss
    y = jnp.concatenate([bb, sb], 0)
    y = y * (0.5 * rank**0.5 / jnp.sqrt(jnp.sum(y * y, keepdims=True)))
    for sweep in range(4):
        product = dot(y, y, ((0,), (0,)), HIGHEST)
        y = 1.5 * y - 0.5 * dot(y, product, ((1,), (0,)), HIGHEST)
    yb = (y[:rank] * sv_col).astype(jnp.bfloat16)
    ys = y[rank:].astype(jnp.bfloat16)
    spread = jnp.where(iota((rank, wide), 1) // n_grp == iota((rank, wide), 0), 1.0, 0.0)
    spread = spread.astype(jnp.bfloat16)
    left_b = dot(spread, yb, ((0,), (1,))).astype(jnp.bfloat16)
    both = dot(left_b, spread, ((1,), (0,)))
    same = lax.rem(iota((wide, wide), 0), n_grp) == lax.rem(iota((wide, wide), 1), n_grp)
    mixb_ref[...] = jnp.where(same, both, 0.0).astype(jnp.bfloat16)
    reps = n_grp * snap
    fill = jnp.where(lax.rem(iota((snap, reps), 1), snap) == iota((snap, reps), 0), 1.0, 0.0)
    left_s = dot(spread, ys, ((0,), (1,))).astype(jnp.bfloat16)
    many = dot(left_s, fill.astype(jnp.bfloat16), ((1,), (0,)))
    same = lax.rem(iota((wide, reps), 0), n_grp) == iota((wide, reps), 1) // snap
    mixs_ref[...] = jnp.where(same, many, 0.0).astype(jnp.bfloat16)

    keep.wait()
    for send in sends:
        send.wait()


def update_kernel(
    gram_in, offset_in, live_hbm, mixb_hbm, mixs_hbm, basis_hbm, snaps_hbm,
    gram_out, offset_out, out_hbm,
    gram_ref, offset_ref, live_ref, mixb_ref, mixs_ref, xb, sb, ob, sem, in_sem, out_sem,
):
    comps, rank, n_grp, capacity = xb.shape
    snap = sb.shape[2]
    planes = capacity // PLANE
    small = []
    pairs = [(mixb_hbm, mixb_ref), (mixs_hbm, mixs_ref), (live_hbm, live_ref)]
    pairs += [(gram_in, gram_ref), (offset_in, offset_ref)]
    for k, (src, dst) in enumerate(pairs):
        small.append(pltpu.make_async_copy(src, dst, sem.at[k]))
        small[-1].start()
    blocks, snap_loads = {}, []
    for c in range(comps):
        load = pltpu.make_async_copy(snaps_hbm.at[:, c], sb.at[c], sem.at[len(pairs) + c])
        load.start()
        snap_loads.append(load)
        for p in range(planes):
            cells = pl.ds(p * PLANE, PLANE)
            load = pltpu.make_async_copy(
                basis_hbm.at[:, c, :, cells], xb.at[c, :, :, cells], in_sem.at[c, p]
            )
            load.start()
            blocks[c, p] = load
    for load in small:
        load.wait()
    outs = [
        pltpu.make_async_copy(gram_ref, gram_out, sem.at[3]),
        pltpu.make_async_copy(offset_ref, offset_out, sem.at[4]),
    ]
    for out in outs:
        out.start()
    live = live_ref[:, :1]
    for c in range(comps):
        snap_loads[c].wait()
        for p in range(planes):
            cells = pl.ds(p * PLANE, PLANE)
            blocks[c, p].wait()
            x = xb[c, :, :, cells].reshape(rank * n_grp, PLANE)
            s = sb[c, :, :, cells].reshape(n_grp * snap, PLANE)
            new = dot(mixb_ref[...], x, ((1,), (0,))) + dot(mixs_ref[...], s, ((1,), (0,)))
            new = jnp.where(p < live, new, 0.0).astype(jnp.bfloat16)
            ob[c, :, :, cells] = new.reshape(rank, n_grp, PLANE)
            out = pltpu.make_async_copy(
                ob.at[c, :, :, cells], out_hbm.at[:, c, :, cells], out_sem.at[c, p]
            )
            out.start()
            outs.append(out)
    for out in outs:
        out.wait()


def per_device(velocity, old_basis, singular_values, thickness):
    snap, comps, _, capacity = velocity.shape
    rank, n_grp = old_basis.shape[0], old_basis.shape[2]
    n_slab = lax.axis_size("slab")
    planes = capacity // PLANE
    wide, reps = rank * n_grp, n_grp * snap
    stages = stages_of(n_slab, n_grp)
    moves = sum(radix - 1 for _, _, radix in stages)
    rows = rank // 2 + snap
    vmem = pl.BlockSpec(memory_space=pltpu.VMEM)
    hbm = pl.BlockSpec(memory_space=pl.ANY)
    gram_matrix, mix_b, mix_s, live, offsets, all_snaps = pl.pallas_call(
        functools.partial(gram_kernel, n_grp, n_slab, stages),
        out_shape=(
            jax.ShapeDtypeStruct((rank + snap, rank + snap), jnp.float32),
            jax.ShapeDtypeStruct((wide, wide), jnp.bfloat16),
            jax.ShapeDtypeStruct((wide, reps), jnp.bfloat16),
            jax.ShapeDtypeStruct((wide, LANES), jnp.float32),
            jax.ShapeDtypeStruct((1, 1), jnp.int32),
            jax.ShapeDtypeStruct((n_grp, comps, snap, capacity), jnp.bfloat16),
        ),
        in_specs=[pl.BlockSpec(memory_space=pltpu.SMEM), vmem, vmem, hbm],
        out_specs=(vmem, vmem, vmem, vmem, vmem, hbm),
        scratch_shapes=[
            pltpu.VMEM((comps, rank, n_grp, capacity), jnp.bfloat16),
            pltpu.VMEM((comps, snap, capacity), jnp.bfloat16),
            pltpu.VMEM((wide // LANES, wide + snap, LANES), jnp.float32),
            pltpu.VMEM((snap, snap), jnp.float32),
            *[pltpu.VMEM((radix, rows, LANES), jnp.float32) for _, _, radix in stages],
            pltpu.SemaphoreType.DMA((comps + 1,)),
            pltpu.SemaphoreType.DMA((comps * (n_grp - 1),)),
            pltpu.SemaphoreType.DMA((comps * (n_grp - 1),)),
            pltpu.SemaphoreType.DMA((moves,)),
            pltpu.SemaphoreType.DMA((moves,)),
        ],
        compiler_params=pltpu.CompilerParams(collective_id=0, has_side_effects=True),
        name="gram_exchange",
    )(thickness, singular_values.reshape(1, rank), velocity, old_basis)
    gram_matrix, offsets, new_basis = pl.pallas_call(
        update_kernel,
        out_shape=(
            jax.ShapeDtypeStruct(gram_matrix.shape, jnp.float32),
            jax.ShapeDtypeStruct((1, 1), jnp.int32),
            jax.ShapeDtypeStruct(old_basis.shape, jnp.bfloat16),
        ),
        in_specs=[hbm] * 7,
        out_specs=(hbm, hbm, hbm),
        scratch_shapes=[
            pltpu.VMEM(gram_matrix.shape, jnp.float32),
            pltpu.VMEM((1, 1), jnp.int32),
            pltpu.VMEM((wide, LANES), jnp.float32),
            pltpu.VMEM((wide, wide), jnp.bfloat16),
            pltpu.VMEM((wide, reps), jnp.bfloat16),
            pltpu.VMEM((comps, rank, n_grp, capacity), jnp.bfloat16),
            pltpu.VMEM((comps, n_grp, snap, capacity), jnp.bfloat16),
            pltpu.VMEM((comps, rank, n_grp, capacity), jnp.bfloat16),
            pltpu.SemaphoreType.DMA((5 + comps,)),
            pltpu.SemaphoreType.DMA((comps, planes)),
            pltpu.SemaphoreType.DMA((comps, planes)),
        ],
        name="basis_update",
    )(gram_matrix, offsets, live, mix_b, mix_s, old_basis, all_snaps)
    return (gram_matrix, new_basis, offsets)


def solution(mesh):
    in_specs = (P(None, None, "grp", "slab"), P(None, None, None, "slab"), P(), P("grp", "slab"))
    out_specs = (P(), P(None, None, None, "slab"), P("grp", "slab"))
    return jax.shard_map(
        per_device, mesh=mesh, in_specs=in_specs, out_specs=out_specs, check_vma=False
    )
```

```python
import functools
import jax
import jax.numpy as jnp
from jax import lax
from jax.experimental import pallas as pl
from jax.experimental.pallas import tpu as pltpu
from jax.sharding import PartitionSpec as P

PLANE = 512
AXES = ("grp", "slab")
MESH = pl.DeviceIdType.MESH
LANES = 128
COUNT_LANE = 32
HIGHEST = lax.Precision.HIGHEST


def stages_of(n_slab, n_grp):
    found = []
    for axis, size, first in (("slab", n_slab, 2), ("grp", n_grp, 4)):
        base, radix = 1, first
        while base < size:
            radix = min(radix, size // base)
            found.append((axis, base, radix))
            base, radix = base * radix, 4
    return found


def partner(axis, base, radix, shift):
    me = {name: lax.axis_index(name) for name in AXES}
    digit = lax.rem(me[axis] // base, radix)
    other = lax.rem(digit + shift, radix)
    me[axis] = me[axis] + (other - digit) * base
    return tuple(me[name] for name in AXES)


def dot(a, b, dims, precision=None):
    return lax.dot_general(
        a, b, (dims, ((), ())), preferred_element_type=jnp.float32, precision=precision
    )


def iota(shape, dim):
    return lax.broadcasted_iota(jnp.int32, shape, dim)


def gram_kernel(
    n_grp, n_slab, stages,
    thick_ref, sv_ref, vel_hbm, basis_ref,
    gram_ref, mixb_ref, mixs_ref, live_ref, offset_ref, all_ref, xb,
    vel_ref, snaps_ref, big, small, *rest,
):
    n_st = len(stages)
    slots = rest[:n_st]
    local_sem, v_send, v_recv, st_send, st_recv = rest[n_st:]
    rank, comps = xb.shape[1], xb.shape[0]
    snap = snaps_ref.shape[1]
    planes = xb.shape[3] // PLANE
    wide = rank * n_grp
    grp, slab = lax.axis_index("grp"), lax.axis_index("slab")

    fetch = pltpu.make_async_copy(vel_hbm, vel_ref, local_sem.at[comps + 1])
    fetch.start()
    loads = []
    for c in range(comps):
        load = pltpu.make_async_copy(basis_ref.at[:, c], xb.at[c], local_sem.at[c])
        load.start()
        loads.append(load)
    barrier = pltpu.get_barrier_semaphore()
    greeted = 0
    for axis, base, radix in stages:
        for shift in range(1, radix):
            pl.semaphore_signal(
                barrier, inc=1, device_id=partner(axis, base, radix, shift), device_id_type=MESH
            )
            greeted += 1
    fetch.wait()
    for c in range(comps):
        snaps_ref[c] = vel_ref[:, c, 0, :].astype(jnp.bfloat16)
    keep = pltpu.make_async_copy(snaps_ref, all_ref.at[grp], local_sem.at[comps])
    keep.start()
    sends = []

    def send_snaps(c):
        for shift in range(1, n_grp):
            at = c * (n_grp - 1) + shift - 1
            send = pltpu.make_async_remote_copy(
                src_ref=snaps_ref.at[c], dst_ref=all_ref.at[grp, c],
                send_sem=v_send.at[at], recv_sem=v_recv.at[at],
                device_id=partner("grp", 1, n_grp, shift), device_id_type=MESH,
            )
            send.start()
            sends.append(send)

    thick = thick_ref[0, 0]
    big[...] = jnp.zeros_like(big)
    small[...] = jnp.zeros_like(small)
    for c in range(comps):
        loads[c].wait()
        for p in range(planes):
            live = jnp.where(p < thick, 1.0, 0.0)
            x = xb[c, :, :, pl.ds(p * PLANE, PLANE)].reshape(wide, PLANE)
            s = snaps_ref[c, :, pl.ds(p * PLANE, PLANE)]
            by_basis = live * dot(x, x, ((1,), (1,)))
            by_snaps = live * dot(s, x, ((1,), (1,)))
            for h in range(wide // LANES):
                big[h, :wide] += by_basis[:, h * LANES : (h + 1) * LANES]
                big[h, wide:] += by_snaps[:, h * LANES : (h + 1) * LANES]
            small[...] += live * dot(s, s, ((1,), (1,)))
        if c == 0:
            pl.semaphore_wait(barrier, greeted)
            for k in range(comps):
                send_snaps(k)
    pick = jnp.where(iota((rank, wide), 1) == iota((rank, wide), 0) * n_grp + grp, 1.0, 0.0)
    mine = [
        jnp.concatenate([big[h, pl.ds(grp, rank, stride=n_grp), :], big[h, wide:]], 0)
        for h in range(wide // LANES)
    ]
    mine = jnp.concatenate(mine, 1)
    right = dot(mine, pick, ((1,), (1,)), HIGHEST)
    bb, sb = right[:rank], right[rank:]
    ss = small[...]
    half, quarter = rank // 2, snap // 2
    rows = half + 2 * quarter
    place = iota((quarter, LANES), 1) - COUNT_LANE
    place = jnp.where(place >= 0, place * quarter + iota((quarter, LANES), 0), -1)
    me = grp * n_slab + slab
    tail = jnp.where(place == me, thick.astype(jnp.float32), 0.0)
    spare = jnp.zeros((quarter, LANES - 2 * snap), jnp.float32)
    tail = tail + jnp.concatenate([ss[:quarter], ss[quarter:], spare], 1)
    total = jnp.concatenate(
        [
            jnp.concatenate([bb[:half], bb[half:]], 1),
            jnp.concatenate([sb[:quarter], sb[quarter:]], 1),
            tail,
        ],
        0,
    )
    sv_row = sv_ref[...]
    eye = iota((rank, rank), 0) == iota((rank, rank), 1)
    sv_col = jnp.sum(jnp.where(eye, sv_row, 0.0), axis=1, keepdims=True)

    at = 0
    for (axis, base, radix), slot in zip(stages, slots):
        digit = lax.rem(lax.axis_index(axis) // base, radix)
        slot[digit] = total
        moves = []
        for shift in range(1, radix):
            move = pltpu.make_async_remote_copy(
                src_ref=slot.at[digit], dst_ref=slot.at[digit],
                send_sem=st_send.at[at], recv_sem=st_recv.at[at],
                device_id=partner(axis, base, radix, shift), device_id_type=MESH,
            )
            move.start()
            moves.append(move)
            at += 1
        for move in moves:
            move.wait()
        total = slot[0]
        for k in range(1, radix):
            total = total + slot[k]

    tail = total[half + quarter :]
    counts = jnp.where(place >= 0, tail, 0.0)
    live_cells = jnp.sum(counts, keepdims=True) * PLANE
    factor = 1.0 / (3.0 * live_cells)
    offset_ref[...] = jnp.sum(jnp.where(place < me, counts, 0.0), keepdims=True).astype(jnp.int32)
    live = jnp.zeros((wide, LANES), jnp.float32)
    region = lax.rem(iota((wide, LANES), 0), n_grp)
    for g in range(n_grp):
        here = jnp.sum(jnp.where(place == g * n_slab + slab, counts, 0.0), keepdims=True)
        live = jnp.where(region == g, here, live)
    live_ref[...] = live

    bb = jnp.concatenate([total[:half, :rank], total[:half, rank:]], 0)
    sb = total[half : half + quarter]
    sb = jnp.concatenate([sb[:, :rank], sb[:, rank:]], 0)
    ss = jnp.concatenate([tail[:, :snap], tail[:, snap : 2 * snap]], 0)
    bb = bb * sv_col * sv_row * factor
    sb = sb * sv_row * factor
    ss = ss * factor
    gram_ref[:rank, :rank] = bb
    gram_ref[rank:, :rank] = sb
    gram_ref[:rank, rank:] = sb.T
    gram_ref[rank:, rank:] = ss
    y = jnp.concatenate([bb, sb], 0)
    y = y * (0.5 * rank**0.5 / jnp.sqrt(jnp.sum(y * y, keepdims=True)))
    for sweep in range(4):
        product = dot(y, y, ((0,), (0,)), HIGHEST)
        y = 1.5 * y - 0.5 * dot(y, product, ((1,), (0,)), HIGHEST)
    yb = (y[:rank] * sv_col).astype(jnp.bfloat16)
    ys = y[rank:].astype(jnp.bfloat16)
    spread = jnp.where(iota((rank, wide), 1) // n_grp == iota((rank, wide), 0), 1.0, 0.0)
    spread = spread.astype(jnp.bfloat16)
    left_b = dot(spread, yb, ((0,), (1,))).astype(jnp.bfloat16)
    both = dot(left_b, spread, ((1,), (0,)))
    same = lax.rem(iota((wide, wide), 0), n_grp) == lax.rem(iota((wide, wide), 1), n_grp)
    mixb_ref[...] = jnp.where(same, both, 0.0).astype(jnp.bfloat16)
    reps = n_grp * snap
    fill = jnp.where(lax.rem(iota((snap, reps), 1), snap) == iota((snap, reps), 0), 1.0, 0.0)
    left_s = dot(spread, ys, ((0,), (1,))).astype(jnp.bfloat16)
    many = dot(left_s, fill.astype(jnp.bfloat16), ((1,), (0,)))
    same = lax.rem(iota((wide, reps), 0), n_grp) == iota((wide, reps), 1) // snap
    mixs_ref[...] = jnp.where(same, many, 0.0).astype(jnp.bfloat16)

    keep.wait()
    for send in sends:
        send.wait()


def update_kernel(
    gram_in, offset_in, live_hbm, mixb_hbm, mixs_hbm, snaps_hbm, xb,
    gram_out, offset_out, out_hbm,
    gram_ref, offset_ref, live_ref, mixb_ref, mixs_ref, sb, ob, sem, out_sem,
):
    comps, rank, n_grp, capacity = xb.shape
    snap = sb.shape[2]
    planes = capacity // PLANE
    small = []
    pairs = [(mixb_hbm, mixb_ref), (mixs_hbm, mixs_ref), (live_hbm, live_ref)]
    pairs += [(gram_in, gram_ref), (offset_in, offset_ref)]
    for k, (src, dst) in enumerate(pairs):
        small.append(pltpu.make_async_copy(src, dst, sem.at[k]))
        small[-1].start()
    snap_loads = []
    for c in range(comps):
        load = pltpu.make_async_copy(snaps_hbm.at[:, c], sb.at[c], sem.at[len(pairs) + c])
        load.start()
        snap_loads.append(load)
    for load in small:
        load.wait()
    outs = [
        pltpu.make_async_copy(gram_ref, gram_out, sem.at[3]),
        pltpu.make_async_copy(offset_ref, offset_out, sem.at[4]),
    ]
    for out in outs:
        out.start()
    live = live_ref[:, :1]
    for c in range(comps):
        snap_loads[c].wait()
        for p in range(planes):
            cells = pl.ds(p * PLANE, PLANE)
            x = xb[c, :, :, cells].reshape(rank * n_grp, PLANE)
            s = sb[c, :, :, cells].reshape(n_grp * snap, PLANE)
            new = dot(mixb_ref[...], x, ((1,), (0,))) + dot(mixs_ref[...], s, ((1,), (0,)))
            new = jnp.where(p < live, new, 0.0).astype(jnp.bfloat16)
            ob[c, :, :, cells] = new.reshape(rank, n_grp, PLANE)
            out = pltpu.make_async_copy(
                ob.at[c, :, :, cells], out_hbm.at[:, c, :, cells], out_sem.at[c, p]
            )
            out.start()
            outs.append(out)
    for out in outs:
        out.wait()


def per_device(velocity, old_basis, singular_values, thickness):
    snap, comps, _, capacity = velocity.shape
    rank, n_grp = old_basis.shape[0], old_basis.shape[2]
    n_slab = lax.axis_size("slab")
    planes = capacity // PLANE
    wide, reps = rank * n_grp, n_grp * snap
    stages = stages_of(n_slab, n_grp)
    moves = sum(radix - 1 for _, _, radix in stages)
    rows = rank // 2 + snap
    vmem = pl.BlockSpec(memory_space=pltpu.VMEM)
    hbm = pl.BlockSpec(memory_space=pl.ANY)
    gram_matrix, mix_b, mix_s, live, offsets, all_snaps, held = pl.pallas_call(
        functools.partial(gram_kernel, n_grp, n_slab, stages),
        out_shape=(
            jax.ShapeDtypeStruct((rank + snap, rank + snap), jnp.float32),
            jax.ShapeDtypeStruct((wide, wide), jnp.bfloat16),
            jax.ShapeDtypeStruct((wide, reps), jnp.bfloat16),
            jax.ShapeDtypeStruct((wide, LANES), jnp.float32),
            jax.ShapeDtypeStruct((1, 1), jnp.int32),
            jax.ShapeDtypeStruct((n_grp, comps, snap, capacity), jnp.bfloat16),
            pltpu.VMEM((comps, rank, n_grp, capacity), jnp.bfloat16),
        ),
        in_specs=[pl.BlockSpec(memory_space=pltpu.SMEM), vmem, hbm, hbm],
        out_specs=(vmem, vmem, vmem, vmem, vmem, hbm, vmem),
        scratch_shapes=[
            pltpu.VMEM(velocity.shape, jnp.float32),
            pltpu.VMEM((comps, snap, capacity), jnp.bfloat16),
            pltpu.VMEM((wide // LANES, wide + snap, LANES), jnp.float32),
            pltpu.VMEM((snap, snap), jnp.float32),
            *[pltpu.VMEM((radix, rows, LANES), jnp.float32) for _, _, radix in stages],
            pltpu.SemaphoreType.DMA((comps + 2,)),
            pltpu.SemaphoreType.DMA((comps * (n_grp - 1),)),
            pltpu.SemaphoreType.DMA((comps * (n_grp - 1),)),
            pltpu.SemaphoreType.DMA((moves,)),
            pltpu.SemaphoreType.DMA((moves,)),
        ],
        compiler_params=pltpu.CompilerParams(collective_id=0, has_side_effects=True),
        name="gram_exchange",
    )(thickness, singular_values.reshape(1, rank), velocity, old_basis)
    held = pltpu.with_memory_space_constraint(held, pltpu.VMEM)
    gram_matrix, offsets, new_basis = pl.pallas_call(
        update_kernel,
        out_shape=(
            jax.ShapeDtypeStruct(gram_matrix.shape, jnp.float32),
            jax.ShapeDtypeStruct((1, 1), jnp.int32),
            jax.ShapeDtypeStruct(old_basis.shape, jnp.bfloat16),
        ),
        in_specs=[hbm] * 6 + [vmem],
        out_specs=(hbm, hbm, hbm),
        scratch_shapes=[
            pltpu.VMEM(gram_matrix.shape, jnp.float32),
            pltpu.VMEM((1, 1), jnp.int32),
            pltpu.VMEM((wide, LANES), jnp.float32),
            pltpu.VMEM((wide, wide), jnp.bfloat16),
            pltpu.VMEM((wide, reps), jnp.bfloat16),
            pltpu.VMEM((comps, n_grp, snap, capacity), jnp.bfloat16),
            pltpu.VMEM((comps, rank, n_grp, capacity), jnp.bfloat16),
            pltpu.SemaphoreType.DMA((5 + comps,)),
            pltpu.SemaphoreType.DMA((comps, planes)),
        ],
        name="basis_update",
    )(gram_matrix, offsets, live, mix_b, mix_s, all_snaps, held)
    return (gram_matrix, new_basis, offsets)


def solution(mesh):
    in_specs = (P(None, None, "grp", "slab"), P(None, None, None, "slab"), P(), P("grp", "slab"))
    out_specs = (P(), P(None, None, None, "slab"), P("grp", "slab"))
    return jax.shard_map(
        per_device, mesh=mesh, in_specs=in_specs, out_specs=out_specs, check_vma=False
    )
```
